32 devices in a mesh: owner: 4 (over x, core), rows: 8 (over z, y).
Axes of the slice: x: 2, y: 2, z: 4, core: 2. Of those that a mesh axis runs over, the one named last changes fastest.
Arguments:
- w_down: float32 [16, 6400, 4096], P('owner', None, 'rows'), may hold values from -0.109375 to 0.109375
- avg_down: bfloat16 [16, 6400, 4096], P('owner', None, 'rows'), may hold values from -0.0390625 to 0.0390625
- router_weight: float32 [4096, 16], P('rows', 'owner'), may hold values from -0.09375 to 0.09375
- router_gain: float32 [4096], P('rows'), may hold values from 0.25 to 1.75
Outputs:
- serve_down: bfloat16 [16, 6400, 4096], P('owner', 'rows')
- scale_down: float32 [16, 6400], P('owner', 'rows')
- serve_router: bfloat16 [4096, 16], replicated
The draws below stay inside these ranges and needn't reach their ends.
All inputs are finite; a program needn't handle non-finite values. Where the reference program divides by a largest or mean magnitude, that divisor is 1e-20 or more.
Results may differ from the reference program's by a relative error of at most 0.001.
Values may be sent and summed in bfloat16 or wider, within the bound.
A program may use at most 256 MiB of HBM per device.

```python
import jax
import jax.numpy as jnp

EXPERTS = 16
D_MODEL = 4096
D_EXPERT = 6400


def strengthened(values, stream_key, source, target, parts, factor):
    def block_of(position):
        return (jnp.arange(values.shape[position]) // (values.shape[position] // parts)).reshape((-1,) + (1,) * (values.ndim - 1 - position))

    one_side = jax.random.permutation(stream_key, parts)[block_of(target)]
    second = (block_of(target) + parts // 2) % parts
    return jnp.where((block_of(source) == one_side) | (block_of(source) == second), factor * values, values)


def shard_levels(rng, dims, cuts, least, high):
    loudness = 1.0
    for dim, parts in cuts:
        draws = jax.random.uniform(jax.random.fold_in(jax.random.fold_in(rng, 6), dim), (parts,), jnp.float32, least / len(cuts), high / len(cuts))
        loudness = loudness * jnp.repeat(jnp.exp(draws), dims[dim] // parts).reshape((-1,) + (1,) * (len(dims) - 1 - dim))
    return loudness


def centred(key, extent, deviation, reach, shards=(), held_as=jnp.bfloat16):
    level = shard_levels(key, extent, shards, -0.22, 0.18) if shards else 1.0
    array = jax.random.normal(key, extent, jnp.float32) * deviation * level
    return jnp.minimum(jnp.maximum(array, -reach), reach).astype(held_as)


def bell_draw_with(stream_key, dims, width, limit, shards, heavy, dtype=jnp.bfloat16):
    result = width * jax.random.normal(stream_key, dims, jnp.float32)
    if shards:
        result = result * shard_levels(stream_key, dims, shards, -0.22, 0.18)
    return jnp.clip(strengthened(result, jax.random.fold_in(stream_key, 3), *heavy), -limit, limit).astype(dtype)


def setup_inputs(seed: int = 0) -> dict:
    seeds = jax.random.split(jax.random.key(seed), 5)
    w_down = bell_draw_with(seeds[0], (EXPERTS, D_EXPERT, D_MODEL), D_EXPERT ** -0.5, 0.109375, ((0, 4), (2, 8)), (2, 1, 8, 2.0), jnp.float32)
    avg_down = centred(seeds[1], (EXPERTS, D_EXPERT, D_MODEL), (D_EXPERT * 4) ** -0.5, 0.0390625, ((0, 4), (2, 8)))
    router_weight = centred(seeds[2], (D_MODEL, EXPERTS), D_MODEL ** -0.5, 0.09375, ((0, 8), (1, 4)), jnp.float32)
    router_gain = jnp.clip(1.0 + 0.15 * jax.random.normal(seeds[3], (D_MODEL,), jnp.float32), 0.25, 1.75)
    return dict(w_down=w_down, avg_down=avg_down, router_weight=router_weight, router_gain=router_gain)


def reference(w_down, avg_down, router_weight, router_gain):
    fresh_down = w_down + avg_down.astype(jnp.float32)
    scale_down = jnp.sum(jnp.abs(fresh_down), axis=2) / D_MODEL
    serve_down = (fresh_down / jnp.expand_dims(scale_down, 2)).astype(jnp.bfloat16)
    serve_router = (router_weight * router_gain[:, None]).astype(jnp.bfloat16)
    return serve_down, scale_down, serve_router
```

```python
import functools

import jax
import jax.numpy as jnp
from jax import lax
from jax.experimental import pallas as pl
from jax.experimental.pallas import tpu as pltpu
from jax.sharding import PartitionSpec as P

LANES = 128
DEPTH = 4
MESH = pl.DeviceIdType.MESH


def kernel(n, owners, tile, w_ref, a_ref, rw_ref, gain_ref, out_ref, scale_ref, router_ref,
           w_buf, a_buf, staged, sums, parts, totals, routed,
           load_sem, own_sem, send_sem, recv_sem, sum_send, sum_recv, tot_send, tot_recv,
           row_send, row_recv, col_send, col_recv):
    me, mine = lax.axis_index("rows"), lax.axis_index("owner")
    experts, rows, cols = w_ref.shape
    block = rows // n
    piece = sums.shape[2]
    per_expert = rows // tile

    def peer(k):
        out, bit = 0, 1
        while bit < n:
            out = out + bit * (((me // bit) % 2 + (k // bit) % 2) % 2)
            bit *= 2
        return out

    def each_peer(fn):
        @pl.loop(1, n)
        def _(k):
            fn(peer(k))

    def each_owner(fn):
        @pl.loop(1, owners)
        def _(k):
            fn((mine + k) % owners)

    barrier = pltpu.get_barrier_semaphore()
    each_peer(lambda p: pl.semaphore_signal(barrier, inc=1, device_id={"rows": p}, device_id_type=MESH))
    each_owner(lambda q: pl.semaphore_signal(barrier, inc=1, device_id={"owner": q}, device_id_type=MESH))

    def loads(first, step):
        slot = step % DEPTH
        e = first + step // per_expert
        span = pl.ds(pl.multiple_of((step % per_expert) * tile, tile), tile)
        return (pltpu.make_async_copy(w_ref.at[e, span], w_buf.at[slot], load_sem.at[0, slot]),
                pltpu.make_async_copy(a_ref.at[e, span], a_buf.at[slot], load_sem.at[1, slot]))

    def prime(first):
        for step in range(DEPTH - 1):
            for copy in loads(first, step):
                copy.start()

    def stream(first, last, body):
        count = (last - first) * per_expert

        @pl.loop(0, count)
        def _(step):
            for copy in loads(first, step):
                copy.wait()

            @pl.when(step + (DEPTH - 1) < count)
            def _():
                for copy in loads(first, step + (DEPTH - 1)):
                    copy.start()

            body(first + step // per_expert, step % per_expert, step % DEPTH)

    def add_up(e, i, slot):
        for j in range(tile // LANES):
            span = slice(j * LANES, (j + 1) * LANES)
            acc = None
            for c in range(0, cols, LANES):
                f = jnp.abs(w_buf[slot, span, c:c + LANES] + a_buf[slot, span, c:c + LANES].astype(jnp.float32))
                acc = f if acc is None else acc + f
            at = i * (tile // LANES) + j
            sums[at // piece, e, pl.ds(at % piece, 1), :] = jnp.sum(acc.T, axis=0, keepdims=True)

    def narrow(e, i, slot):
        for j in range(tile // LANES):
            span = slice(j * LANES, (j + 1) * LANES)
            at = i * (tile // LANES) + j
            inverse = 1.0 / totals[at // piece, e, pl.ds(at % piece, 1), :]
            factor = jnp.broadcast_to(inverse, (LANES, LANES)).T
            where = pl.ds(pl.multiple_of(i * tile + j * LANES, LANES), LANES)
            for c in range(0, cols, LANES):
                f = w_buf[slot, span, c:c + LANES] + a_buf[slot, span, c:c + LANES].astype(jnp.float32)
                staged[e, where, c:c + LANES] = (f * factor).astype(jnp.bfloat16)

    def sum_copy(g, span, p, source):
        return pltpu.make_async_remote_copy(
            src_ref=sums.at[p, span], dst_ref=parts.at[source, span],
            send_sem=sum_send.at[g, p], recv_sem=sum_recv.at[g, source],
            device_id={"rows": p}, device_id_type=MESH)

    def total_copy(g, span, p, source):
        return pltpu.make_async_remote_copy(
            src_ref=totals.at[source, span], dst_ref=totals.at[source, span],
            send_sem=tot_send.at[g, p], recv_sem=tot_recv.at[g, source],
            device_id={"rows": p}, device_id_type=MESH)

    def exchange(g, first, last):
        span = pl.ds(first, last - first)
        each_peer(lambda p: sum_copy(g, span, p, me).start())
        parts[me, first:last] = sums[me, first:last]
        each_peer(lambda p: sum_copy(g, span, p, p).wait_recv())
        total = parts[0, first:last]
        for r in range(1, n):
            total = total + parts[r, first:last]
        totals[me, first:last] = total / (cols * n)
        each_peer(lambda p: total_copy(g, span, p, me).start())
        each_peer(lambda p: total_copy(g, span, p, p).wait_recv())

    def block_copy(e, p, source):
        return pltpu.make_async_remote_copy(
            src_ref=staged.at[e, pl.ds(pl.multiple_of(p * block, 16), block)],
            dst_ref=out_ref.at[e, :, pl.ds(pl.multiple_of(source * cols, LANES), cols)],
            send_sem=send_sem.at[e, p], recv_sem=recv_sem.at[e, source],
            device_id={"rows": p}, device_id_type=MESH)

    def own_copy(e):
        return pltpu.make_async_copy(
            staged.at[e, pl.ds(pl.multiple_of(me * block, 16), block)],
            out_ref.at[e, :, pl.ds(pl.multiple_of(me * cols, LANES), cols)],
            own_sem.at[e])

    def row_copy(p, source):
        return pltpu.make_async_remote_copy(
            src_ref=routed.at[mine, source], dst_ref=routed.at[mine, source],
            send_sem=row_send.at[p], recv_sem=row_recv.at[source],
            device_id={"rows": p}, device_id_type=MESH)

    def col_copy(q, source):
        return pltpu.make_async_remote_copy(
            src_ref=routed.at[source], dst_ref=routed.at[source],
            send_sem=col_send.at[q], recv_sem=col_recv.at[source],
            device_id={"owner": q}, device_id_type=MESH)

    prime(0)
    sums[...] = jnp.zeros_like(sums)
    routed[mine, me] = (rw_ref[...] * gain_ref[...]).astype(jnp.bfloat16)
    stream(0, 1, add_up)
    prime(0)
    pl.semaphore_wait(barrier, n - 1 + owners - 1)

    exchange(0, 0, 1)
    stream(0, 1, narrow)
    early = n // 2
    block_copy(0, peer(early), me).start()
    if experts > 1:
        prime(1)
    each_peer(lambda p: row_copy(p, me).start())
    own_copy(0).start()

    if experts > 1:
        stream(1, experts, add_up)
        prime(1)
        exchange(1, 1, experts)

    @pl.loop(1, n - 1)
    def _(k):
        block_copy(0, peer(k + k // early), me).start()

    each_peer(lambda p: row_copy(p, p).wait_recv())
    each_owner(lambda q: col_copy(q, mine).start())

    for e in range(1, experts):
        stream(e, e + 1, narrow)
        if e + 1 < experts:
            prime(e + 1)
        each_peer(lambda p, e=e: block_copy(e, p, me).start())
        own_copy(e).start()

    each_owner(lambda q: col_copy(q, q).wait_recv())
    scale_ref[...] = totals[...]
    router_ref[...] = routed[...]

    each_owner(lambda q: col_copy(q, mine).wait_send())
    each_peer(lambda p: row_copy(p, me).wait_send())
    for g, (first, last) in enumerate([(0, 1), (1, experts)][:min(experts, 2)]):
        span = pl.ds(first, last - first)
        each_peer(lambda p, g=g, span=span: sum_copy(g, span, p, me).wait_send())
        each_peer(lambda p, g=g, span=span: total_copy(g, span, p, me).wait_send())
    for e in range(experts):
        own_copy(e).wait()
        each_peer(lambda p, e=e: block_copy(e, p, me).wait_send())
        each_peer(lambda p, e=e: block_copy(e, p, p).wait_recv())


def with_kernel(n, owners, w_down, avg_down, router_weight, router_gain):
    experts, rows, cols = w_down.shape
    lane_rows = rows // LANES
    tile = LANES * max(t for t in range(1, 6) if lane_rows % t == 0)
    piece = -(-lane_rows // n)
    few = router_weight.shape[1]
    block = rows // n
    pair = pltpu.SemaphoreType.DMA((2, n))
    out, totals, routed = pl.pallas_call(
        functools.partial(kernel, n, owners, tile),
        out_shape=(
            jax.ShapeDtypeStruct((experts, block, cols * n), jnp.bfloat16),
            jax.ShapeDtypeStruct((n, experts, piece, LANES), jnp.float32),
            jax.ShapeDtypeStruct((owners, n, few, cols), jnp.bfloat16),
        ),
        in_specs=[pl.BlockSpec(memory_space=pl.ANY)] * 2 + [pl.BlockSpec(memory_space=pltpu.VMEM)] * 2,
        out_specs=(
            pl.BlockSpec(memory_space=pl.ANY),
            pl.BlockSpec(memory_space=pltpu.VMEM),
            pl.BlockSpec(memory_space=pltpu.VMEM),
        ),
        scratch_shapes=[
            pltpu.VMEM((DEPTH, tile, cols), jnp.float32),
            pltpu.VMEM((DEPTH, tile, cols), jnp.bfloat16),
            pltpu.VMEM((experts, rows, cols), jnp.bfloat16),
            pltpu.VMEM((n, experts, piece, LANES), jnp.float32),
            pltpu.VMEM((n, experts, piece, LANES), jnp.float32),
            pltpu.VMEM((n, experts, piece, LANES), jnp.float32),
            pltpu.VMEM((owners, n, few, cols), jnp.bfloat16),
            pltpu.SemaphoreType.DMA((2, DEPTH)),
            pltpu.SemaphoreType.DMA((experts,)),
            pltpu.SemaphoreType.DMA((experts, n)),
            pltpu.SemaphoreType.DMA((experts, n)),
            pair, pair, pair, pair,
            pltpu.SemaphoreType.DMA((n,)),
            pltpu.SemaphoreType.DMA((n,)),
            pltpu.SemaphoreType.DMA((owners,)),
            pltpu.SemaphoreType.DMA((owners,)),
        ],
        compiler_params=pltpu.CompilerParams(
            collective_id=0, has_side_effects=True, vmem_limit_bytes=60000 * 1024
        ),
        name="serve",
    )(w_down, avg_down, router_weight.T, router_gain[None, :])
    scales = jnp.transpose(totals, (1, 0, 2, 3)).reshape(experts, -1)
    scales = lax.dynamic_slice_in_dim(scales, lax.axis_index("rows") * block, block, axis=1)
    router = jnp.transpose(routed, (0, 2, 1, 3)).reshape(owners * few, n * cols).T
    return out, scales, router


def with_collectives(n, owners, w_down, avg_down, router_weight, router_gain):
    fresh = w_down + avg_down.astype(jnp.float32)
    scales = lax.psum(jnp.sum(jnp.abs(fresh), axis=2), "rows") / (w_down.shape[2] * n)
    narrow = (fresh / jnp.expand_dims(scales, 2)).astype(jnp.bfloat16)
    out = lax.all_to_all(narrow, "rows", split_axis=1, concat_axis=2, tiled=True)
    scales = lax.dynamic_slice_in_dim(scales, lax.axis_index("rows") * out.shape[1], out.shape[1], axis=1)
    part = (router_weight * router_gain[:, None]).astype(jnp.bfloat16)
    router = lax.all_gather(lax.all_gather(part, "rows", axis=0, tiled=True), "owner", axis=1, tiled=True)
    return out, scales, router


def solution(mesh):
    n, owners = mesh.shape["rows"], mesh.shape["owner"]

    def per_device(w_down, avg_down, router_weight, router_gain):
        experts, rows, cols = w_down.shape
        fits = (n & (n - 1)) == 0 and rows % LANES == 0 and rows % (16 * n) == 0 and cols % LANES == 0
        path = with_kernel if fits else with_collectives
        return path(n, owners, w_down, avg_down, router_weight, router_gain)

    return jax.shard_map(
        per_device,
        mesh=mesh,
        in_specs=(
            P("owner", None, "rows"),
            P("owner", None, "rows"),
            P("rows", "owner"),
            P("rows"),
        ),
        out_specs=(P("owner", "rows", None), P("owner", "rows"), P()),
        check_vma=False,
    )
```
